32 devices in a mesh: section: 4 (over z), shard: 8 (over y, x, core).
Axes of the slice: x: 2, y: 2, z: 4, core: 2. Of those that a mesh axis runs over, the one named last changes fastest.
Arguments:
- grad_parts: bfloat16 [4, 8, 256, 8192], P('section', 'shard'), may hold values from -6 to 6
- params: bfloat16 [4, 256, 8192], P('section', 'shard'), may hold values from -6 to 6
- moment_first: float32 [4, 256, 8192], P('section', 'shard'), may hold values from -6 to 6
- moment_second: float32 [4, 256, 8192], P('section', 'shard'), may hold values from 0.5 to 50
- block_layer: int32 [4, 32], P('section', 'shard'), may hold values from 0 to 7, as said below
- block_valid: int32 [4, 32], P('section', 'shard'), may hold values from 0 to 1
- decay: float32 [8], replicated, may hold values from 0.05 to 1
Outputs:
- new_params: bfloat16 [4, 256, 8192], P('section', 'shard')
- new_first: float32 [4, 256, 8192], P('section', 'shard')
- new_second: float32 [4, 256, 8192], P('section', 'shard')
- ratios: float32 [8], replicated
The draws below stay inside these ranges and needn't reach their ends.
Inputs may be any that keep to these rules, and one draw needn't show every extreme that they name: `block_layer`: in every section the live slots come first. One section has all 32 slots live; each other section has between 16 and 32 live slots, and all sections together have 3 * 32. Over the live slots taken section by section in order, layer ids never fall and every layer has exactly 12 live slots; dead slots hold arbitrary layer ids.
All inputs are finite; a program needn't handle non-finite values.
Results may differ from the reference program's by a relative error of at most 0.008.
Values may be sent and summed in bfloat16 or wider, within the bound.
A program may use at most 64 MiB of HBM per device.

```python
import math
import jax
import jax.numpy as jnp
from jax import lax

D = 8192
LAYERS = 8
BLOCK = 8
SECTION_BLK = 32
SECTION_ROWS = 256
LAYER_BLK = 12
N_SECTION = 4
N_SHARD = 8


def layout(key):
    keyed = jax.random.fold_in(key, 11)
    full = SECTION_BLK
    half_blk = SECTION_BLK // 2
    first_count = jax.random.randint(jax.random.fold_in(keyed, 3), (), half_blk, full + 1)
    lower = jnp.maximum(half_blk, full - first_count)
    upper = jnp.minimum(full, 3 * half_blk - first_count)
    second_count = jax.random.randint(jax.random.fold_in(keyed, 4), (), lower, upper + 1)
    third_count = 2 * full - first_count - second_count
    base = jnp.stack([jnp.array(full, jnp.int32), first_count.astype(jnp.int32), second_count.astype(jnp.int32), third_count.astype(jnp.int32)])
    order = jax.random.permutation(jax.random.fold_in(keyed, 1), 4)
    counts = base[order]
    offsets = jnp.cumsum(counts) - counts
    slots = jnp.arange(SECTION_BLK, dtype=jnp.int32)
    valid = slots[None, :] < counts[:, None]
    position = offsets[:, None] + slots[None, :]
    layer = position // LAYER_BLK
    filler = jax.random.randint(jax.random.fold_in(keyed, 2), (4, SECTION_BLK), 0, LAYERS)
    return (jnp.where(valid, layer, filler).astype(jnp.int32), valid.astype(jnp.int32))


def draw_block_layer(key, part):
    return layout(key)[0]


def draw_block_valid(key, part):
    return layout(key)[1]


def strengthened(result, key, source, target, blocks, factor):
    owner, partner = [(jnp.arange(result.shape[dim]) // (result.shape[dim] // blocks)).reshape([-1 if axis == dim else 1 for axis in range(result.ndim)]) for dim in (source, target)]
    chosen = jax.random.permutation(key, blocks)[partner]
    strong = (owner == chosen) | (owner == (partner + blocks // 2) % blocks)
    return jnp.where(strong, factor * result, result)


def level_of(own_key, shape, shards, least, top_value):
    factor_of, own = 1.0, jax.random.fold_in(own_key, 6)
    for axis_at, blocks in shards:
        heights = jnp.exp(jax.random.uniform(jax.random.fold_in(own, axis_at), (blocks,), jnp.float32, least / len(shards), top_value / len(shards)))
        factor_of = factor_of * jnp.repeat(heights, shape[axis_at] // blocks).reshape([-1 if axis == axis_at else 1 for axis in range(len(shape))])
    return factor_of


def centred(stream_key, shape, spread, bound, split=(), kind=jnp.bfloat16):
    loudness = level_of(stream_key, shape, split, -0.22, 0.18) if split else 1.0
    result = jax.random.normal(stream_key, shape, jnp.float32) * spread * loudness
    return jnp.minimum(jnp.maximum(result, -bound), bound).astype(kind)


def noise_with(key, dims, width, bound, pieces, heavy, kind=jnp.bfloat16):
    entries = width * jax.random.normal(key, dims, jnp.float32)
    if pieces:
        entries = entries * level_of(key, dims, pieces, -0.22, 0.18)
    return jnp.clip(strengthened(entries, jax.random.fold_in(key, 3), *heavy), -bound, bound).astype(kind)


def setup_inputs(seed: int = 0) -> dict:
    seeds = jax.random.split(jax.random.key(seed), 8)
    return {
        "grad_parts": noise_with(seeds[0], (N_SECTION, N_SHARD, SECTION_ROWS, D), 1.0, 6.0, ((0, 4), (1, 8)), (1, 2, 8, 2.0)),
        "params": centred(seeds[1], (N_SECTION, SECTION_ROWS, D), 1.0, 6.0, ((0, 4), (1, 8))),
        "moment_first": centred(seeds[2], (N_SECTION, SECTION_ROWS, D), 1.0, 6.0, ((0, 4), (1, 8)), jnp.float32),
        "moment_second": jnp.clip(jnp.exp(math.log(50.0) - 4.6051702 * jax.random.uniform(seeds[3], (N_SECTION, SECTION_ROWS, D), jnp.float32) ** level_of(seeds[3], (N_SECTION, SECTION_ROWS, D), ((0, 4), (1, 8)), -0.2, 0.2)), 0.5, 50.0),
        "block_layer": draw_block_layer(jax.random.fold_in(seeds[7], 71), 0),
        "block_valid": draw_block_valid(jax.random.fold_in(seeds[7], 71), 0),
        "decay": jnp.clip(jnp.exp(jax.random.uniform(seeds[6], (LAYERS,), jnp.float32, math.log(0.05), math.log(1.0))), 0.05, 1.0),
    }


bias_first = 1.0 - 0.9 ** 10
bias_second = 1.0 - 0.99 ** 10

def reference(grad_parts, params, moment_first, moment_second, block_layer, block_valid, decay):

    def add_part(index, running):
        return running + lax.dynamic_index_in_dim(grad_parts, index, 1, keepdims=False).astype(jnp.float32)
    initial = jnp.zeros((grad_parts.shape[0], grad_parts.shape[2], grad_parts.shape[3]), jnp.float32)
    gradient = lax.fori_loop(0, grad_parts.shape[1], add_part, initial)
    first = 0.9 * moment_first + 0.1 * gradient
    second = 0.99 * moment_second + 0.01 * gradient * gradient
    layer_rows = jnp.repeat(block_layer, BLOCK, axis=1)
    valid_rows = jnp.repeat(block_valid, BLOCK, axis=1) > 0
    weights = params.astype(jnp.float32)
    update = first / bias_first / (jnp.sqrt(second / bias_second) + 1e-06) + decay[layer_rows][..., None] * weights
    onehot = jnp.where(valid_rows[..., None] & (layer_rows[..., None] == jnp.arange(LAYERS, dtype=jnp.int32)), 1.0, 0.0).astype(jnp.float32)
    weight_sq = lax.optimization_barrier(jnp.sum(weights * weights, axis=-1))
    update_sq = lax.optimization_barrier(jnp.sum(update * update, axis=-1))
    wsum = jnp.einsum('sr,srl->l', weight_sq, onehot, precision=lax.Precision.HIGHEST)
    usum = jnp.einsum('sr,srl->l', update_sq, onehot, precision=lax.Precision.HIGHEST)
    ratios = jnp.sqrt(wsum / (usum + 1.0))
    row_ratio = ratios[layer_rows]
    stepped = weights - 0.1 * row_ratio[..., None] * update
    new_params = jnp.where(valid_rows[..., None], stepped, weights).astype(jnp.bfloat16)
    new_first = jnp.where(valid_rows[..., None], first, moment_first)
    new_second = jnp.where(valid_rows[..., None], second, moment_second)
    return (new_params, new_first, new_second, ratios)
```

```python
import functools
import math

import jax
import jax.numpy as jnp
from jax import lax
from jax.experimental import pallas as pl
from jax.experimental.pallas import tpu as pltpu
from jax.sharding import PartitionSpec as P

MESH = pl.DeviceIdType.MESH
bias_first = 1.0 - 0.9**10
bias_second = 1.0 - 0.99**10
LANES = 128
PIECES = 8


def kernel(
    n_sec, n_y, n_x, pieces,
    g_hbm, p_hbm, m1_hbm, m2_hbm, layer_ref, valid_ref, decay_ref,
    newp_ref, new1_ref, new2_ref, ratio_ref,
    own, away, d2d, p_v, m1_v, m2_v, upd, r1a, r1b, s1a, s1b, r2a, r2b, tiles, ztiles,
    load_sem, state_sem, pair_sem, one_send, one_recv, two_send, two_recv,
    t_send, t_recv, z_send, z_recv,
):
    rows, cols = p_v.shape
    width = cols // pieces
    n_shard = 2 * n_y * n_x
    sec, me = lax.axis_index("section"), lax.axis_index("shard")
    core = lax.rem(me, 2)
    x = lax.rem(me // 2, n_x)
    y = me // (2 * n_x)
    blocks = layer_ref.shape[1]
    block_rows = rows // blocks

    def at(yy, xx, cc):
        return (sec, (yy * n_x + xx) * 2 + cc)

    def span(p):
        return pl.ds(p * width, width)

    loads = []
    for p in range(pieces):
        a = pltpu.make_async_copy(g_hbm.at[:, :, 1 - core, :, span(p)], away.at[:, :, :, span(p)], load_sem.at[0, p])
        b = pltpu.make_async_copy(g_hbm.at[:, :, core, :, span(p)], own.at[:, :, :, span(p)], load_sem.at[1, p])
        a.start()
        b.start()
        loads.append((a, b))
    states = [
        pltpu.make_async_copy(src, dst, state_sem.at[i])
        for i, (src, dst) in enumerate(((p_hbm, p_v), (m1_hbm, m1_v), (m2_hbm, m2_v)))
    ]
    for s in states:
        s.start()

    barrier = pltpu.get_barrier_semaphore()
    for j in range(1, n_shard):
        pl.semaphore_signal(barrier, inc=1, device_id=(sec, lax.rem(me + j, n_shard)), device_id_type=MESH)
    for j in range(1, n_sec):
        pl.semaphore_signal(barrier, inc=1, device_id=(lax.rem(sec + j, n_sec), me), device_id_type=MESH)
    pl.semaphore_wait(barrier, n_shard - 1 + n_sec - 1)

    pair = []
    for p in range(pieces):
        loads[p][0].wait()
        c = pltpu.make_async_remote_copy(
            src_ref=away.at[:, :, :, span(p)], dst_ref=d2d.at[:, :, :, span(p)],
            send_sem=pair_sem.at[0, p], recv_sem=pair_sem.at[1, p],
            device_id=at(y, x, 1 - core), device_id_type=MESH,
        )
        c.start()
        pair.append(c)

    ones = []
    for p in range(pieces):
        loads[p][1].wait()
        pair[p].wait_recv()

        def add_pair(i, carry, p=p):
            yy, xx = i // n_x, lax.rem(i, n_x)
            total = own[yy, xx, :, span(p)].astype(jnp.float32) + d2d[yy, xx, :, span(p)].astype(jnp.float32)
            own[yy, xx, :, span(p)] = total.astype(jnp.bfloat16)
            return carry

        lax.fori_loop(0, n_y * n_x, add_pair, 0)
        group = []
        along_x = p % 2 == 0
        for j in range(1, n_x if along_x else n_y):
            if along_x:
                t = lax.rem(x + j, n_x)
                src, dst, dev = own.at[:, t, :, span(p)], r1a.at[p // 2, j - 1], at(y, t, core)
            else:
                t = lax.rem(y + j, n_y)
                src, dst, dev = own.at[t, :, :, span(p)], r1b.at[p // 2, j - 1], at(t, x, core)
            c = pltpu.make_async_remote_copy(
                src_ref=src, dst_ref=dst,
                send_sem=one_send.at[p, j - 1], recv_sem=one_recv.at[p, j - 1],
                device_id=dev, device_id_type=MESH,
            )
            c.start()
            group.append(c)
        ones.append(group)

    twos = []
    for p in range(pieces):
        for c in ones[p]:
            c.wait_recv()
        group = []
        along_x = p % 2 == 0
        for j in range(1, n_y if along_x else n_x):
            if along_x:
                t = lax.rem(y + j, n_y)
                total = own[t, x, :, span(p)].astype(jnp.float32)
                for k in range(n_x - 1):
                    total += r1a[p // 2, k, t].astype(jnp.float32)
                s1a[p // 2, j - 1] = total.astype(jnp.bfloat16)
                src, dst, dev = s1a.at[p // 2, j - 1], r2a.at[p // 2, j - 1], at(t, x, core)
            else:
                t = lax.rem(x + j, n_x)
                total = own[y, t, :, span(p)].astype(jnp.float32)
                for k in range(n_y - 1):
                    total += r1b[p // 2, k, t].astype(jnp.float32)
                s1b[p // 2, j - 1] = total.astype(jnp.bfloat16)
                src, dst, dev = s1b.at[p // 2, j - 1], r2b.at[p // 2, j - 1], at(y, t, core)
            c = pltpu.make_async_remote_copy(
                src_ref=src, dst_ref=dst,
                send_sem=two_send.at[p, j - 1], recv_sem=two_recv.at[p, j - 1],
                device_id=dev, device_id_type=MESH,
            )
            c.start()
            group.append(c)
        twos.append(group)

    def by_block(scalars):
        return jnp.concatenate([jnp.full((block_rows, LANES), s) for s in scalars], axis=0)

    layers = [layer_ref[0, b] for b in range(blocks)]
    lives = [valid_ref[0, b] for b in range(blocks)]
    row_decay = by_block([decay_ref[layer] for layer in layers])
    row_live = by_block([jnp.where(v > 0, 1.0, 0.0).astype(jnp.float32) for v in lives]) > 0.5

    for s in states:
        s.wait()

    zero = jnp.zeros((rows, LANES), jnp.float32)
    sums = (zero, zero)
    for p in range(pieces):
        for c in twos[p]:
            c.wait_recv()
        along_x = p % 2 == 0

        def update_piece(i, sums, p=p, along_x=along_x):
            usum, wsum = sums
            inner = pl.ds(pl.multiple_of(i * LANES, LANES), LANES)
            outer = pl.ds(pl.multiple_of(p * width + i * LANES, LANES), LANES)
            grad = own[y, x, :, outer].astype(jnp.float32)
            if along_x:
                for k in range(n_x - 1):
                    grad += r1a[p // 2, k, y, :, inner].astype(jnp.float32)
                for k in range(n_y - 1):
                    grad += r2a[p // 2, k, :, inner].astype(jnp.float32)
            else:
                for k in range(n_y - 1):
                    grad += r1b[p // 2, k, x, :, inner].astype(jnp.float32)
                for k in range(n_x - 1):
                    grad += r2b[p // 2, k, :, inner].astype(jnp.float32)
            weights = p_v[:, outer].astype(jnp.float32)
            old1, old2 = m1_v[:, outer], m2_v[:, outer]
            first = 0.9 * old1 + 0.1 * grad
            second = 0.99 * old2 + 0.01 * grad * grad
            update = first / bias_first / (jnp.sqrt(second / bias_second) + 1e-06) + row_decay * weights
            upd[:, outer] = update
            new1_ref[:, outer] = jnp.where(row_live, first, old1)
            new2_ref[:, outer] = jnp.where(row_live, second, old2)
            return usum + update * update, wsum + weights * weights

        sums = lax.fori_loop(0, width // LANES, update_piece, sums, unroll=2)

    n_layer = decay_ref.shape[0]
    layer_iota = lax.broadcasted_iota(jnp.int32, (n_layer, LANES), 0)
    for q in range(2):
        tile = jnp.zeros((n_layer, LANES), jnp.float32)
        for b in range(blocks):
            line = jnp.sum(sums[q][b * block_rows : (b + 1) * block_rows], axis=0, keepdims=True)
            chosen = jnp.where(lives[b] > 0, layers[b], -1)
            tile += jnp.where(layer_iota == chosen, line, 0.0)
        tiles[me, q] = tile
    sends = []
    for j in range(1, n_shard):
        t = lax.rem(me + j, n_shard)
        c = pltpu.make_async_remote_copy(
            src_ref=tiles.at[me], dst_ref=tiles.at[me],
            send_sem=t_send.at[j - 1], recv_sem=t_recv.at[j - 1],
            device_id=(sec, t), device_id_type=MESH,
        )
        c.start()
        sends.append(c)
    for c in sends:
        c.wait_recv()
    total = tiles[0]
    for j in range(1, n_shard):
        total += tiles[j]
    ztiles[sec] = total
    zsends = []
    for j in range(1, n_sec):
        c = pltpu.make_async_remote_copy(
            src_ref=ztiles.at[sec], dst_ref=ztiles.at[sec],
            send_sem=z_send.at[j - 1], recv_sem=z_recv.at[j - 1],
            device_id=(lax.rem(sec + j, n_sec), me), device_id_type=MESH,
        )
        c.start()
        zsends.append(c)
    for c in zsends:
        c.wait_recv()
    total = ztiles[0]
    for j in range(1, n_sec):
        total += ztiles[j]
    totals = jnp.sum(total, axis=-1, keepdims=True)
    ratios = jnp.sqrt(totals[1] / (totals[0] + 1.0))
    ratio_tile = jnp.broadcast_to(ratios, (n_layer, LANES))
    ratio_ref[...] = ratio_tile
    row_step = jnp.concatenate(
        [
            jnp.broadcast_to(
                0.1 * jnp.sum(
                    jnp.where((layer_iota == layers[b]) & (layer_iota >= 0) & (lives[b] > 0), ratio_tile, 0.0),
                    axis=0, keepdims=True,
                ),
                (block_rows, LANES),
            )
            for b in range(blocks)
        ],
        axis=0,
    )

    def step_piece(i, carry):
        outer = pl.ds(pl.multiple_of(i * LANES, LANES), LANES)
        weights = p_v[:, outer].astype(jnp.float32)
        stepped = weights - row_step * upd[:, outer]
        newp_ref[:, outer] = jnp.where(row_live, stepped, weights).astype(jnp.bfloat16)
        return carry

    lax.fori_loop(0, cols // LANES, step_piece, 0, unroll=4)

    for c in pair + [c for group in ones + twos for c in group] + sends + zsends:
        c.wait_send()


def shards(grad_parts, params, moment_first, moment_second, block_layer, block_valid, decay):
    n_sec, n_shard = lax.axis_size("section"), lax.axis_size("shard")
    chips = n_shard // 2
    n_y = max(d for d in range(1, math.isqrt(chips) + 1) if chips % d == 0)
    n_x = chips // n_y
    rows, cols = params.shape[1:]
    n_layer = decay.shape[0]
    pieces = PIECES
    half, width = pieces // 2, cols // pieces
    bf16, f32 = jnp.bfloat16, jnp.float32
    dma = pltpu.SemaphoreType.DMA
    most = max(n_x, n_y) - 1
    grads = grad_parts.reshape(n_y, n_x, 2, rows, cols)
    any_spec = pl.BlockSpec(memory_space=pl.ANY)
    smem = pl.BlockSpec(memory_space=pltpu.SMEM)
    vmem = pl.BlockSpec(memory_space=pltpu.VMEM)
    new_params, new_first, new_second, ratio = pl.pallas_call(
        functools.partial(kernel, n_sec, n_y, n_x, pieces),
        out_shape=(
            OUT((rows, cols), bf16),
            OUT((rows, cols), f32),
            OUT((rows, cols), f32),
            jax.ShapeDtypeStruct((n_layer, LANES), f32),
        ),
        in_specs=[any_spec] * 4 + [smem] * 3,
        out_specs=(vmem, vmem, vmem, vmem),
        scratch_shapes=[
            pltpu.VMEM((n_y, n_x, rows, cols), bf16),
            pltpu.VMEM((n_y, n_x, rows, cols), bf16),
            pltpu.VMEM((n_y, n_x, rows, cols), bf16),
            pltpu.VMEM((rows, cols), bf16),
            pltpu.VMEM((rows, cols), f32),
            pltpu.VMEM((rows, cols), f32),
            pltpu.VMEM((rows, cols), f32),
            pltpu.VMEM((half, n_x - 1, n_y, rows, width), bf16),
            pltpu.VMEM((half, n_y - 1, n_x, rows, width), bf16),
            pltpu.VMEM((half, n_y - 1, rows, width), bf16),
            pltpu.VMEM((half, n_x - 1, rows, width), bf16),
            pltpu.VMEM((half, n_y - 1, rows, width), bf16),
            pltpu.VMEM((half, n_x - 1, rows, width), bf16),
            pltpu.VMEM((n_shard, 2, n_layer, LANES), f32),
            pltpu.VMEM((n_sec, 2, n_layer, LANES), f32),
            dma((2, pieces)),
            dma((3,)),
            dma((2, pieces)),
            dma((pieces, most)),
            dma((pieces, most)),
            dma((pieces, most)),
            dma((pieces, most)),
            dma((n_shard - 1,)),
            dma((n_shard - 1,)),
            dma((n_sec - 1,)),
            dma((n_sec - 1,)),
        ],
        compiler_params=pltpu.CompilerParams(
            collective_id=0, has_side_effects=True, vmem_limit_bytes=56 * 1024 * 1024
        ),
    )(grads, params[0], moment_first[0], moment_second[0], block_layer, block_valid, decay)
    return (new_params[None], new_first[None], new_second[None], ratio[:, 0])


OUT = jax.ShapeDtypeStruct


def solution(mesh):
    placed = (
        P("section", "shard", None, None),
        P("section", "shard", None),
        P("section", "shard", None),
        P("section", "shard", None),
        P("section", "shard"),
        P("section", "shard"),
        P(),
    )
    return jax.shard_map(
        shards,
        mesh=mesh,
        in_specs=placed,
        out_specs=(
            P("section", "shard", None),
            P("section", "shard", None),
            P("section", "shard", None),
            P(),
        ),
        check_vma=False,
    )
```

```python
import functools
import math

import jax
import jax.numpy as jnp
from jax import lax
from jax.experimental import pallas as pl
from jax.experimental.pallas import tpu as pltpu
from jax.sharding import PartitionSpec as P

MESH = pl.DeviceIdType.MESH
bias_first = 1.0 - 0.9**10
bias_second = 1.0 - 0.99**10
LANES = 128
PIECES = 8
ONE_SHOT = True


def kernel(
    n_sec, n_y, n_x, pieces,
    g_hbm, p_hbm, m1_hbm, m2_hbm, layer_ref, valid_ref, decay_ref,
    newp_ref, new1_ref, new2_ref, ratio_ref,
    own, away, d2d, p_v, m1_v, m2_v, upd, r1a, r1b, s1a, s1b, r2a, r2b, tiles, ztiles,
    load_sem, state_sem, pair_sem, one_send, one_recv, two_send, two_recv,
    t_send, t_recv, z_send, z_recv,
):
    rows, cols = p_v.shape
    width = cols // pieces
    n_shard = 2 * n_y * n_x
    sec, me = lax.axis_index("section"), lax.axis_index("shard")
    core = lax.rem(me, 2)
    x = lax.rem(me // 2, n_x)
    y = me // (2 * n_x)
    blocks = layer_ref.shape[1]
    block_rows = rows // blocks

    def at(yy, xx, cc):
        return (sec, (yy * n_x + xx) * 2 + cc)

    def span(p):
        return pl.ds(p * width, width)

    loads = []
    for p in range(pieces):
        a = pltpu.make_async_copy(g_hbm.at[:, :, 1 - core, :, span(p)], away.at[:, :, :, span(p)], load_sem.at[0, p])
        b = pltpu.make_async_copy(g_hbm.at[:, :, core, :, span(p)], own.at[:, :, :, span(p)], load_sem.at[1, p])
        a.start()
        b.start()
        loads.append((a, b))
    states = [
        pltpu.make_async_copy(src, dst, state_sem.at[i])
        for i, (src, dst) in enumerate(((p_hbm, p_v), (m1_hbm, m1_v), (m2_hbm, m2_v)))
    ]
    for s in states:
        s.start()

    barrier = pltpu.get_barrier_semaphore()
    for j in range(1, n_shard):
        pl.semaphore_signal(barrier, inc=1, device_id=(sec, lax.rem(me + j, n_shard)), device_id_type=MESH)
    for i in range(1, n_sec):
        for j in range(n_shard if ONE_SHOT and n_shard * n_sec <= 32 else 1):
            peer = (lax.rem(sec + i, n_sec), lax.rem(me + j, n_shard))
            pl.semaphore_signal(barrier, inc=1, device_id=peer, device_id_type=MESH)
    pl.semaphore_wait(barrier, n_shard - 1 + (n_sec - 1) * (n_shard if ONE_SHOT and n_shard * n_sec <= 32 else 1))

    pair = []
    for p in range(pieces):
        loads[p][0].wait()
        c = pltpu.make_async_remote_copy(
            src_ref=away.at[:, :, :, span(p)], dst_ref=d2d.at[:, :, :, span(p)],
            send_sem=pair_sem.at[0, p], recv_sem=pair_sem.at[1, p],
            device_id=at(y, x, 1 - core), device_id_type=MESH,
        )
        c.start()
        pair.append(c)

    ones = []
    for p in range(pieces):
        loads[p][1].wait()
        pair[p].wait_recv()

        def add_pair(i, carry, p=p):
            yy, xx = i // n_x, lax.rem(i, n_x)
            total = own[yy, xx, :, span(p)].astype(jnp.float32) + d2d[yy, xx, :, span(p)].astype(jnp.float32)
            own[yy, xx, :, span(p)] = total.astype(jnp.bfloat16)
            return carry

        lax.fori_loop(0, n_y * n_x, add_pair, 0)
        group = []
        along_x = p % 2 == 0
        for j in range(1, n_x if along_x else n_y):
            if along_x:
                t = lax.rem(x + j, n_x)
                src, dst, dev = own.at[:, t, :, span(p)], r1a.at[p // 2, j - 1], at(y, t, core)
            else:
                t = lax.rem(y + j, n_y)
                src, dst, dev = own.at[t, :, :, span(p)], r1b.at[p // 2, j - 1], at(t, x, core)
            c = pltpu.make_async_remote_copy(
                src_ref=src, dst_ref=dst,
                send_sem=one_send.at[p, j - 1], recv_sem=one_recv.at[p, j - 1],
                device_id=dev, device_id_type=MESH,
            )
            c.start()
            group.append(c)
        ones.append(group)

    twos = []
    for p in range(pieces):
        for c in ones[p]:
            c.wait_recv()
        group = []
        along_x = p % 2 == 0
        for j in range(1, n_y if along_x else n_x):
            if along_x:
                t = lax.rem(y + j, n_y)
                total = own[t, x, :, span(p)].astype(jnp.float32)
                for k in range(n_x - 1):
                    total += r1a[p // 2, k, t].astype(jnp.float32)
                s1a[p // 2, j - 1] = total.astype(jnp.bfloat16)
                src, dst, dev = s1a.at[p // 2, j - 1], r2a.at[p // 2, j - 1], at(t, x, core)
            else:
                t = lax.rem(x + j, n_x)
                total = own[y, t, :, span(p)].astype(jnp.float32)
                for k in range(n_y - 1):
                    total += r1b[p // 2, k, t].astype(jnp.float32)
                s1b[p // 2, j - 1] = total.astype(jnp.bfloat16)
                src, dst, dev = s1b.at[p // 2, j - 1], r2b.at[p // 2, j - 1], at(y, t, core)
            c = pltpu.make_async_remote_copy(
                src_ref=src, dst_ref=dst,
                send_sem=two_send.at[p, j - 1], recv_sem=two_recv.at[p, j - 1],
                device_id=dev, device_id_type=MESH,
            )
            c.start()
            group.append(c)
        twos.append(group)

    def by_block(scalars):
        return jnp.concatenate([jnp.full((block_rows, LANES), s) for s in scalars], axis=0)

    layers = [layer_ref[0, b] for b in range(blocks)]
    lives = [valid_ref[0, b] for b in range(blocks)]
    row_decay = by_block([decay_ref[layer] for layer in layers])
    row_live = by_block([jnp.where(v > 0, 1.0, 0.0).astype(jnp.float32) for v in lives]) > 0.5

    for s in states:
        s.wait()

    zero = jnp.zeros((rows, LANES), jnp.float32)
    sums = (zero, zero)
    for p in range(pieces):
        for c in twos[p]:
            c.wait_recv()
        along_x = p % 2 == 0

        def update_piece(i, sums, p=p, along_x=along_x):
            usum, wsum = sums
            inner = pl.ds(pl.multiple_of(i * LANES, LANES), LANES)
            outer = pl.ds(pl.multiple_of(p * width + i * LANES, LANES), LANES)
            grad = own[y, x, :, outer].astype(jnp.float32)
            if along_x:
                for k in range(n_x - 1):
                    grad += r1a[p // 2, k, y, :, inner].astype(jnp.float32)
                for k in range(n_y - 1):
                    grad += r2a[p // 2, k, :, inner].astype(jnp.float32)
            else:
                for k in range(n_y - 1):
                    grad += r1b[p // 2, k, x, :, inner].astype(jnp.float32)
                for k in range(n_x - 1):
                    grad += r2b[p // 2, k, :, inner].astype(jnp.float32)
            weights = p_v[:, outer].astype(jnp.float32)
            old1, old2 = m1_v[:, outer], m2_v[:, outer]
            first = 0.9 * old1 + 0.1 * grad
            second = 0.99 * old2 + 0.01 * grad * grad
            update = first / bias_first / (jnp.sqrt(second / bias_second) + 1e-06) + row_decay * weights
            upd[:, outer] = update
            new1_ref[:, outer] = jnp.where(row_live, first, old1)
            new2_ref[:, outer] = jnp.where(row_live, second, old2)
            return usum + update * update, wsum + weights * weights

        sums = lax.fori_loop(0, width // LANES, update_piece, sums, unroll=2)

    n_layer = decay_ref.shape[0]
    lane = lax.broadcasted_iota(jnp.int32, (1, LANES), 1)
    line = jnp.zeros((1, LANES), jnp.float32)
    for b in range(blocks):
        chosen = jnp.where(lives[b] > 0, layers[b], -LANES)
        for q, values in enumerate((sums[1], sums[0])):
            part = jnp.sum(values[b * block_rows : (b + 1) * block_rows], axis=0, keepdims=True)
            line += jnp.where(lane == chosen + q * n_layer, jnp.sum(part, axis=1, keepdims=True), 0.0)

    def all_sum(line, slots, send_sem, recv_sem, index, peers):
        slots[index] = line
        copies = []
        for j, peer in enumerate(peers):
            c = pltpu.make_async_remote_copy(
                src_ref=slots.at[index], dst_ref=slots.at[index],
                send_sem=send_sem.at[j], recv_sem=recv_sem.at[j],
                device_id=peer, device_id_type=MESH,
            )
            c.start()
            copies.append(c)
        for c in copies:
            c.wait_recv()
        total = slots[0]
        for j in range(1, len(peers) + 1):
            total += slots[j]
        return total, copies

    shard_peers = [(sec, lax.rem(me + j, n_shard)) for j in range(1, n_shard)]
    sec_peers = [(lax.rem(sec + j, n_sec), me) for j in range(1, n_sec)]
    if ONE_SHOT and n_shard * n_sec <= 32:
        every = [
            (lax.rem(sec + i, n_sec), lax.rem(me + j, n_shard))
            for i in range(n_sec) for j in range(n_shard) if i or j
        ]
        line, sends = all_sum(line, tiles, t_send, t_recv, sec * n_shard + me, every[::-1])
    else:
        line, sends = all_sum(line, tiles, t_send, t_recv, me, shard_peers)
        line, zsends = all_sum(line, ztiles, z_send, z_recv, sec, sec_peers)
        sends += zsends
    ratios = jnp.sqrt(line / (pltpu.roll(line, LANES - n_layer, 1) + 1.0))
    ratio_ref[...] = ratios
    row_step = jnp.concatenate(
        [
            jnp.broadcast_to(
                0.1 * jnp.sum(jnp.where(lane == layers[b], ratios, 0.0), axis=1, keepdims=True),
                (block_rows, LANES),
            )
            for b in range(blocks)
        ],
        axis=0,
    )

    def step_piece(i, carry):
        outer = pl.ds(pl.multiple_of(i * LANES, LANES), LANES)
        weights = p_v[:, outer].astype(jnp.float32)
        stepped = weights - row_step * upd[:, outer]
        newp_ref[:, outer] = jnp.where(row_live, stepped, weights).astype(jnp.bfloat16)
        return carry

    lax.fori_loop(0, cols // LANES, step_piece, 0, unroll=4)

    for c in pair + [c for group in ones + twos for c in group] + sends:
        c.wait_send()


def finish(newp_v, new1_v, new2_v, ratio_v, newp_hbm, new1_hbm, new2_hbm, ratio_ref, sem):
    copies = [
        pltpu.make_async_copy(src, dst, sem.at[i])
        for i, (src, dst) in enumerate(((new1_v, new1_hbm), (new2_v, new2_hbm), (newp_v, newp_hbm)))
    ]
    for c in copies:
        c.start()
    ratio_ref[...] = ratio_v[0, : ratio_ref.shape[0]]
    for c in copies:
        c.wait()


def shards(grad_parts, params, moment_first, moment_second, block_layer, block_valid, decay):
    n_sec, n_shard = lax.axis_size("section"), lax.axis_size("shard")
    chips = n_shard // 2
    n_y = max(d for d in range(1, math.isqrt(chips) + 1) if chips % d == 0)
    n_x = chips // n_y
    rows, cols = params.shape[1:]
    n_layer = decay.shape[0]
    pieces = PIECES
    half, width = pieces // 2, cols // pieces
    bf16, f32 = jnp.bfloat16, jnp.float32
    dma = pltpu.SemaphoreType.DMA
    n_lines = n_shard * n_sec if ONE_SHOT and n_shard * n_sec <= 32 else n_shard
    most = max(n_x, n_y) - 1
    grads = grad_parts.reshape(n_y, n_x, 2, rows, cols)
    any_spec = pl.BlockSpec(memory_space=pltpu.HBM)
    smem = pl.BlockSpec(memory_space=pltpu.SMEM)
    vmem = pl.BlockSpec(memory_space=pltpu.VMEM)
    new_params, new_first, new_second, ratio = pl.pallas_call(
        functools.partial(kernel, n_sec, n_y, n_x, pieces),
        out_shape=(
            pltpu.VMEM((rows, cols), bf16),
            pltpu.VMEM((rows, cols), f32),
            pltpu.VMEM((rows, cols), f32),
            pltpu.VMEM((1, LANES), f32),
        ),
        in_specs=[any_spec] * 4 + [smem] * 3,
        out_specs=(vmem, vmem, vmem, vmem),
        scratch_shapes=[
            pltpu.VMEM((n_y, n_x, rows, cols), bf16),
            pltpu.VMEM((n_y, n_x, rows, cols), bf16),
            pltpu.VMEM((n_y, n_x, rows, cols), bf16),
            pltpu.VMEM((rows, cols), bf16),
            pltpu.VMEM((rows, cols), f32),
            pltpu.VMEM((rows, cols), f32),
            pltpu.VMEM((rows, cols), f32),
            pltpu.VMEM((half, n_x - 1, n_y, rows, width), bf16),
            pltpu.VMEM((half, n_y - 1, n_x, rows, width), bf16),
            pltpu.VMEM((half, n_y - 1, rows, width), bf16),
            pltpu.VMEM((half, n_x - 1, rows, width), bf16),
            pltpu.VMEM((half, n_y - 1, rows, width), bf16),
            pltpu.VMEM((half, n_x - 1, rows, width), bf16),
            pltpu.VMEM((n_lines, 1, LANES), f32),
            pltpu.VMEM((n_sec, 1, LANES), f32),
            dma((2, pieces)),
            dma((3,)),
            dma((2, pieces)),
            dma((pieces, most)),
            dma((pieces, most)),
            dma((pieces, most)),
            dma((pieces, most)),
            dma((n_lines - 1,)),
            dma((n_lines - 1,)),
            dma((n_sec - 1,)),
            dma((n_sec - 1,)),
        ],
        compiler_params=pltpu.CompilerParams(
            collective_id=0, has_side_effects=True, vmem_limit_bytes=60 * 1024 * 1024
        ),
    )(grads, params[0], moment_first[0], moment_second[0], block_layer, block_valid, decay)
    out = pl.pallas_call(
        finish,
        out_shape=(
            jax.ShapeDtypeStruct((rows, cols), bf16),
            jax.ShapeDtypeStruct((rows, cols), f32),
            jax.ShapeDtypeStruct((rows, cols), f32),
            jax.ShapeDtypeStruct((n_layer,), f32),
        ),
        in_specs=[vmem] * 4,
        out_specs=(any_spec, any_spec, any_spec, vmem),
        scratch_shapes=[dma((3,))],
        compiler_params=pltpu.CompilerParams(vmem_limit_bytes=8 * 1024 * 1024),
    )(new_params, new_first, new_second, ratio)
    return (out[0][None], out[1][None], out[2][None], out[3])


def solution(mesh):
    placed = (
        P("section", "shard", None, None),
        P("section", "shard", None),
        P("section", "shard", None),
        P("section", "shard", None),
        P("section", "shard"),
        P("section", "shard"),
        P(),
    )
    return jax.shard_map(
        shards,
        mesh=mesh,
        in_specs=placed,
        out_specs=(
            P("section", "shard", None),
            P("section", "shard", None),
            P("section", "shard", None),
            P(),
        ),
        check_vma=False,
    )
```

```python
import functools
import math

import jax
import jax.numpy as jnp
from jax import lax
from jax.experimental import pallas as pl
from jax.experimental.pallas import tpu as pltpu
from jax.sharding import PartitionSpec as P

MESH = pl.DeviceIdType.MESH
bias_first = 1.0 - 0.9**10
bias_second = 1.0 - 0.99**10
LANES = 128
PIECES = 8
ONE_SHOT = True
PARTS = 2


def kernel(
    n_sec, n_y, n_x, pieces,
    g_hbm, p_hbm, m1_hbm, m2_hbm, layer_ref, valid_ref, decay_ref,
    p_v, upd, new1_ref, new2_ref, step_ref, ratio_ref,
    own, away, d2d, m1_v, m2_v, r1a, r1b, s1a, s1b, r2a, r2b, tiles, ztiles,
    load_sem, state_sem, pair_sem, one_send, one_recv, two_send, two_recv,
    t_send, t_recv, z_send, z_recv, told,
):
    rows, cols = p_v.shape
    width = cols // pieces
    n_shard = 2 * n_y * n_x
    sec, me = lax.axis_index("section"), lax.axis_index("shard")
    core = lax.rem(me, 2)
    x = lax.rem(me // 2, n_x)
    y = me // (2 * n_x)
    blocks = layer_ref.shape[1]
    block_rows = rows // blocks

    def at(yy, xx, cc):
        return (sec, (yy * n_x + xx) * 2 + cc)

    def span(p):
        return pl.ds(p * width, width)

    loads = []
    for p in range(pieces):
        a = pltpu.make_async_copy(g_hbm.at[:, :, 1 - core, :, span(p)], away.at[:, :, :, span(p)], load_sem.at[0, p])
        b = pltpu.make_async_copy(g_hbm.at[:, :, core, :, span(p)], own.at[:, :, :, span(p)], load_sem.at[1, p])
        a.start()
        b.start()
        loads.append((a, b))
    states = [
        pltpu.make_async_copy(src, dst, state_sem.at[i])
        for i, (src, dst) in enumerate(((p_hbm, p_v), (m1_hbm, m1_v), (m2_hbm, m2_v)))
    ]
    for s in states:
        s.start()

    barrier = pltpu.get_barrier_semaphore()
    near = [at(y, x, 1 - core)]
    near += [at(y, lax.rem(x + j, n_x), core) for j in range(1, n_x)]
    near += [at(lax.rem(y + j, n_y), x, core) for j in range(1, n_y)]
    for peer in near:
        pl.semaphore_signal(barrier, inc=1, device_id=peer, device_id_type=MESH)
    last_sec = n_sec - 1
    up = (jnp.minimum(sec + 1, last_sec), me)
    down = (jnp.maximum(sec - 1, 0), me)

    @pl.when(sec < last_sec)
    def _():
        pl.semaphore_signal(barrier, inc=1, device_id=up, device_id_type=MESH)

    @pl.when(sec > 0)
    def _():
        pl.semaphore_signal(barrier, inc=1, device_id=down, device_id_type=MESH)

    ends = jnp.where(sec < last_sec, 1, 0) + jnp.where(sec > 0, 1, 0)
    pl.semaphore_wait(barrier, len(near) + ends)

    def relay(d):
        if d > 1:

            @pl.when(sec >= d - 1)
            def _():
                pl.semaphore_wait(told.at[0, d - 2], 1)

            @pl.when(sec <= n_sec - d)
            def _():
                pl.semaphore_wait(told.at[1, d - 2], 1)

        if d < n_sec:

            @pl.when((sec >= d - 1) & (sec < last_sec))
            def _():
                pl.semaphore_signal(told.at[0, d - 1], inc=1, device_id=up, device_id_type=MESH)

            @pl.when((sec <= n_sec - d) & (sec > 0))
            def _():
                pl.semaphore_signal(told.at[1, d - 1], inc=1, device_id=down, device_id_type=MESH)

    pair = []
    for p in range(pieces):
        loads[p][0].wait()
        c = pltpu.make_async_remote_copy(
            src_ref=away.at[:, :, :, span(p)], dst_ref=d2d.at[:, :, :, span(p)],
            send_sem=pair_sem.at[0, p], recv_sem=pair_sem.at[1, p],
            device_id=at(y, x, 1 - core), device_id_type=MESH,
        )
        c.start()
        pair.append(c)

    ones = []
    for p in range(pieces):
        loads[p][1].wait()
        pair[p].wait_recv()

        def add_pair(i, carry, p=p):
            yy, xx = i // n_x, lax.rem(i, n_x)
            total = own[yy, xx, :, span(p)].astype(jnp.float32) + d2d[yy, xx, :, span(p)].astype(jnp.float32)
            own[yy, xx, :, span(p)] = total.astype(jnp.bfloat16)
            return carry

        lax.fori_loop(0, n_y * n_x, add_pair, 0)
        group = []
        along_x = p % 2 == 0
        for j in range(1, n_x if along_x else n_y):
            if along_x:
                t = lax.rem(x + j, n_x)
                src, dst, dev = own.at[:, t, :, span(p)], r1a.at[p // 2, j - 1], at(y, t, core)
            else:
                t = lax.rem(y + j, n_y)
                src, dst, dev = own.at[t, :, :, span(p)], r1b.at[p // 2, j - 1], at(t, x, core)
            c = pltpu.make_async_remote_copy(
                src_ref=src, dst_ref=dst,
                send_sem=one_send.at[p, j - 1], recv_sem=one_recv.at[p, j - 1],
                device_id=dev, device_id_type=MESH,
            )
            c.start()
            group.append(c)
        ones.append(group)

    twos = []
    for p in range(pieces):
        for c in ones[p]:
            c.wait_recv()
        group = []
        along_x = p % 2 == 0
        for j in range(1, n_y if along_x else n_x):
            if along_x:
                t = lax.rem(y + j, n_y)
                total = own[t, x, :, span(p)].astype(jnp.float32)
                for k in range(n_x - 1):
                    total += r1a[p // 2, k, t].astype(jnp.float32)
                s1a[p // 2, j - 1] = total.astype(jnp.bfloat16)
                src, dst, dev = s1a.at[p // 2, j - 1], r2a.at[p // 2, j - 1], at(t, x, core)
            else:
                t = lax.rem(x + j, n_x)
                total = own[y, t, :, span(p)].astype(jnp.float32)
                for k in range(n_y - 1):
                    total += r1b[p // 2, k, t].astype(jnp.float32)
                s1b[p // 2, j - 1] = total.astype(jnp.bfloat16)
                src, dst, dev = s1b.at[p // 2, j - 1], r2b.at[p // 2, j - 1], at(y, t, core)
            c = pltpu.make_async_remote_copy(
                src_ref=src, dst_ref=dst,
                send_sem=two_send.at[p, j - 1], recv_sem=two_recv.at[p, j - 1],
                device_id=dev, device_id_type=MESH,
            )
            c.start()
            group.append(c)
        twos.append(group)

    def by_block(scalars):
        return jnp.concatenate([jnp.full((block_rows, LANES), s) for s in scalars], axis=0)

    layers = [layer_ref[0, b] for b in range(blocks)]
    lives = [valid_ref[0, b] for b in range(blocks)]
    row_decay = by_block([decay_ref[layer] for layer in layers])
    row_live = by_block([jnp.where(v > 0, 1.0, 0.0).astype(jnp.float32) for v in lives]) > 0.5

    for s in states:
        s.wait()

    zero = jnp.zeros((rows, LANES), jnp.float32)
    sums = (zero, zero)
    for p in range(pieces):
        for c in twos[p]:
            c.wait_recv()
        along_x = p % 2 == 0

        def update_piece(i, sums, p=p, along_x=along_x):
            usum, wsum = sums
            inner = pl.ds(pl.multiple_of(i * LANES, LANES), LANES)
            outer = pl.ds(pl.multiple_of(p * width + i * LANES, LANES), LANES)
            grad = own[y, x, :, outer].astype(jnp.float32)
            if along_x:
                for k in range(n_x - 1):
                    grad += r1a[p // 2, k, y, :, inner].astype(jnp.float32)
                for k in range(n_y - 1):
                    grad += r2a[p // 2, k, :, inner].astype(jnp.float32)
            else:
                for k in range(n_y - 1):
                    grad += r1b[p // 2, k, x, :, inner].astype(jnp.float32)
                for k in range(n_x - 1):
                    grad += r2b[p // 2, k, :, inner].astype(jnp.float32)
            weights = p_v[:, outer].astype(jnp.float32)
            old1, old2 = m1_v[:, outer], m2_v[:, outer]
            first = 0.9 * old1 + 0.1 * grad
            second = 0.99 * old2 + 0.01 * grad * grad
            update = first * (1.0 / bias_first) / (jnp.sqrt(second * (1.0 / bias_second)) + 1e-06) + row_decay * weights
            upd[:, outer] = update
            new1_ref[:, outer] = jnp.where(row_live, first, old1)
            new2_ref[:, outer] = jnp.where(row_live, second, old2)
            return usum + update * update, wsum + weights * weights

        sums = lax.fori_loop(0, width // LANES, update_piece, sums, unroll=2)
        if p < n_sec:
            relay(p + 1)

    for d in range(pieces, n_sec):
        relay(d + 1)

    n_layer = decay_ref.shape[0]
    lane = lax.broadcasted_iota(jnp.int32, (1, LANES), 1)
    line = jnp.zeros((1, LANES), jnp.float32)
    for b in range(blocks):
        chosen = jnp.where(lives[b] > 0, layers[b], -LANES)
        for q, values in enumerate((sums[1], sums[0])):
            part = jnp.sum(values[b * block_rows : (b + 1) * block_rows], axis=0, keepdims=True)
            line += jnp.where(lane == chosen + q * n_layer, jnp.sum(part, axis=1, keepdims=True), 0.0)

    def all_sum(line, slots, send_sem, recv_sem, index, peers):
        slots[index] = line
        copies = []
        for j, peer in enumerate(peers):
            c = pltpu.make_async_remote_copy(
                src_ref=slots.at[index], dst_ref=slots.at[index],
                send_sem=send_sem.at[j], recv_sem=recv_sem.at[j],
                device_id=peer, device_id_type=MESH,
            )
            c.start()
            copies.append(c)
        for c in copies:
            c.wait_recv()
        total = slots[0]
        for j in range(1, len(peers) + 1):
            total += slots[j]
        return total, copies

    shard_peers = [(sec, lax.rem(me + j, n_shard)) for j in range(1, n_shard)]
    sec_peers = [(lax.rem(sec + j, n_sec), me) for j in range(1, n_sec)]
    if ONE_SHOT and n_shard * n_sec <= 32:
        every = [
            (lax.rem(sec + i, n_sec), lax.rem(me + j, n_shard))
            for i in range(n_sec) for j in range(n_shard) if i or j
        ]
        line, sends = all_sum(line, tiles, t_send, t_recv, sec * n_shard + me, every[::-1])
    else:
        line, sends = all_sum(line, tiles, t_send, t_recv, me, shard_peers)
        line, zsends = all_sum(line, ztiles, z_send, z_recv, sec, sec_peers)
        sends += zsends
    ratios = jnp.sqrt(line / (pltpu.roll(line, LANES - n_layer, 1) + 1.0))
    ratio_ref[...] = ratios
    step_ref[...] = jnp.concatenate(
        [
            jnp.broadcast_to(
                0.1 * jnp.sum(
                    jnp.where((lane == layers[b]) & (lives[b] > 0), ratios, 0.0), axis=1, keepdims=True
                ),
                (block_rows, LANES),
            )
            for b in range(blocks)
        ],
        axis=0,
    )

    for c in pair + [c for group in ones + twos for c in group] + sends:
        c.wait_send()


def finish(parts, p_v, upd, new1_v, new2_v, step_v, ratio_v, newp_hbm, new1_hbm, new2_hbm, ratio_ref, newp_v, sem):
    cols = p_v.shape[1]
    width = cols // parts
    copies = []
    for k in range(parts):
        span = pl.ds(k * width, width)
        for i, (src, dst) in enumerate(((new1_v, new1_hbm), (new2_v, new2_hbm))):
            c = pltpu.make_async_copy(src.at[:, span], dst.at[:, span], sem.at[i, k])
            c.start()
            copies.append(c)
    ratio_ref[...] = ratio_v[0, : ratio_ref.shape[0]]
    row_step = step_v[...]

    for k in range(parts):
        def step_piece(i, carry, k=k):
            outer = pl.ds(pl.multiple_of(k * width + i * LANES, LANES), LANES)
            stepped = p_v[:, outer].astype(jnp.float32) - row_step * upd[:, outer]
            newp_v[:, outer] = stepped.astype(jnp.bfloat16)
            return carry

        lax.fori_loop(0, width // LANES, step_piece, 0, unroll=4)
        span = pl.ds(k * width, width)
        c = pltpu.make_async_copy(newp_v.at[:, span], newp_hbm.at[:, span], sem.at[2, k])
        c.start()
        copies.append(c)
    for c in copies:
        c.wait()


def shards(grad_parts, params, moment_first, moment_second, block_layer, block_valid, decay):
    n_sec, n_shard = lax.axis_size("section"), lax.axis_size("shard")
    chips = n_shard // 2
    n_y = max(d for d in range(1, math.isqrt(chips) + 1) if chips % d == 0)
    n_x = chips // n_y
    rows, cols = params.shape[1:]
    n_layer = decay.shape[0]
    pieces = PIECES
    half, width = pieces // 2, cols // pieces
    bf16, f32 = jnp.bfloat16, jnp.float32
    dma = pltpu.SemaphoreType.DMA
    n_lines = n_shard * n_sec if ONE_SHOT and n_shard * n_sec <= 32 else n_shard
    most = max(n_x, n_y) - 1
    grads = grad_parts.reshape(n_y, n_x, 2, rows, cols)
    any_spec = pl.BlockSpec(memory_space=pltpu.HBM)
    smem = pl.BlockSpec(memory_space=pltpu.SMEM)
    vmem = pl.BlockSpec(memory_space=pltpu.VMEM)
    held = pl.pallas_call(
        functools.partial(kernel, n_sec, n_y, n_x, pieces),
        out_shape=(
            pltpu.VMEM((rows, cols), bf16),
            pltpu.VMEM((rows, cols), f32),
            pltpu.VMEM((rows, cols), f32),
            pltpu.VMEM((rows, cols), f32),
            pltpu.VMEM((rows, LANES), f32),
            pltpu.VMEM((1, LANES), f32),
        ),
        in_specs=[any_spec] * 4 + [smem] * 3,
        out_specs=(vmem,) * 6,
        scratch_shapes=[
            pltpu.VMEM((n_y, n_x, rows, cols), bf16),
            pltpu.VMEM((n_y, n_x, rows, cols), bf16),
            pltpu.VMEM((n_y, n_x, rows, cols), bf16),
            pltpu.VMEM((rows, cols), f32),
            pltpu.VMEM((rows, cols), f32),
            pltpu.VMEM((half, n_x - 1, n_y, rows, width), bf16),
            pltpu.VMEM((half, n_y - 1, n_x, rows, width), bf16),
            pltpu.VMEM((half, n_y - 1, rows, width), bf16),
            pltpu.VMEM((half, n_x - 1, rows, width), bf16),
            pltpu.VMEM((half, n_y - 1, rows, width), bf16),
            pltpu.VMEM((half, n_x - 1, rows, width), bf16),
            pltpu.VMEM((n_lines, 1, LANES), f32),
            pltpu.VMEM((n_sec, 1, LANES), f32),
            dma((2, pieces)),
            dma((3,)),
            dma((2, pieces)),
            dma((pieces, most)),
            dma((pieces, most)),
            dma((pieces, most)),
            dma((pieces, most)),
            dma((n_lines - 1,)),
            dma((n_lines - 1,)),
            dma((n_sec - 1,)),
            dma((n_sec - 1,)),
            pltpu.SemaphoreType.REGULAR((2, n_sec - 1)),
        ],
        compiler_params=pltpu.CompilerParams(
            collective_id=0, has_side_effects=True, vmem_limit_bytes=56 * 1024 * 1024
        ),
    )(grads, params[0], moment_first[0], moment_second[0], block_layer, block_valid, decay)
    out = pl.pallas_call(
        functools.partial(finish, PARTS),
        out_shape=(
            jax.ShapeDtypeStruct((rows, cols), bf16),
            jax.ShapeDtypeStruct((rows, cols), f32),
            jax.ShapeDtypeStruct((rows, cols), f32),
            jax.ShapeDtypeStruct((n_layer,), f32),
        ),
        in_specs=[vmem] * 6,
        out_specs=(any_spec, any_spec, any_spec, vmem),
        scratch_shapes=[pltpu.VMEM((rows, cols), bf16), dma((3, PARTS))],
        compiler_params=pltpu.CompilerParams(vmem_limit_bytes=8 * 1024 * 1024),
    )(*held)
    return (out[0][None], out[1][None], out[2][None], out[3])


def solution(mesh):
    placed = (
        P("section", "shard", None, None),
        P("section", "shard", None),
        P("section", "shard", None),
        P("section", "shard", None),
        P("section", "shard"),
        P("section", "shard"),
        P(),
    )
    return jax.shard_map(
        shards,
        mesh=mesh,
        in_specs=placed,
        out_specs=(
            P("section", "shard", None),
            P("section", "shard", None),
            P("section", "shard", None),
            P(),
        ),
        check_vma=False,
    )
```

```python
import functools
import math

import jax
import jax.numpy as jnp
from jax import lax
from jax.experimental import pallas as pl
from jax.experimental.pallas import tpu as pltpu
from jax.sharding import PartitionSpec as P

MESH = pl.DeviceIdType.MESH
bias_first = 1.0 - 0.9**10
bias_second = 1.0 - 0.99**10
LANES = 128
PIECES = 8
ONE_SHOT = True
PARTS = 2


def kernel(
    n_sec, n_y, n_x, pieces,
    g_hbm, p_hbm, m1_hbm, m2_hbm, layer_ref, valid_ref, decay_ref,
    p_v, upd, new1_ref, new2_ref, step_ref, ratio_ref,
    own, away, d2d, m1_v, m2_v, r1a, r1b, s1a, s1b, r2a, r2b, tiles, ztiles,
    load_sem, state_sem, pair_sem, one_send, one_recv, two_send, two_recv,
    t_send, t_recv, z_send, z_recv, told, xa, xb, raw_send, raw_recv,
):
    rows, cols = p_v.shape
    width = cols // pieces
    raw = xa.shape[-1]
    n_shard = 2 * n_y * n_x
    sec, me = lax.axis_index("section"), lax.axis_index("shard")
    core = lax.rem(me, 2)
    x = lax.rem(me // 2, n_x)
    y = me // (2 * n_x)
    blocks = layer_ref.shape[1]
    block_rows = rows // blocks

    def at(yy, xx, cc):
        return (sec, (yy * n_x + xx) * 2 + cc)

    def span(p):
        return pl.ds(p * width, width)

    loads = []
    for p in range(pieces):
        a = pltpu.make_async_copy(g_hbm.at[:, :, 1 - core, :, span(p)], away.at[:, :, :, span(p)], load_sem.at[0, p])
        b = pltpu.make_async_copy(g_hbm.at[:, :, core, :, span(p)], own.at[:, :, :, span(p)], load_sem.at[1, p])
        a.start()
        b.start()
        loads.append((a, b))
    states = [
        pltpu.make_async_copy(src, dst, state_sem.at[i])
        for i, (src, dst) in enumerate(((p_hbm, p_v), (m1_hbm, m1_v), (m2_hbm, m2_v)))
    ]
    for s in states:
        s.start()

    barrier = pltpu.get_barrier_semaphore()
    near = [at(y, x, 1 - core)]
    for cc in (core, 1 - core):
        near += [at(y, lax.rem(x + j, n_x), cc) for j in range(1, n_x)]
        near += [at(lax.rem(y + j, n_y), x, cc) for j in range(1, n_y)]
    for peer in near:
        pl.semaphore_signal(barrier, inc=1, device_id=peer, device_id_type=MESH)
    last_sec = n_sec - 1
    up = (jnp.minimum(sec + 1, last_sec), me)
    down = (jnp.maximum(sec - 1, 0), me)

    @pl.when(sec < last_sec)
    def _():
        pl.semaphore_signal(barrier, inc=1, device_id=up, device_id_type=MESH)

    @pl.when(sec > 0)
    def _():
        pl.semaphore_signal(barrier, inc=1, device_id=down, device_id_type=MESH)

    ends = jnp.where(sec < last_sec, 1, 0) + jnp.where(sec > 0, 1, 0)
    pl.semaphore_wait(barrier, len(near) + ends)

    def relay(d):
        if d > 1:

            @pl.when(sec >= d - 1)
            def _():
                pl.semaphore_wait(told.at[0, d - 2], 1)

            @pl.when(sec <= n_sec - d)
            def _():
                pl.semaphore_wait(told.at[1, d - 2], 1)

        if d < n_sec:

            @pl.when((sec >= d - 1) & (sec < last_sec))
            def _():
                pl.semaphore_signal(told.at[0, d - 1], inc=1, device_id=up, device_id_type=MESH)

            @pl.when((sec <= n_sec - d) & (sec > 0))
            def _():
                pl.semaphore_signal(told.at[1, d - 1], inc=1, device_id=down, device_id_type=MESH)

    def raw_span(p):
        return pl.ds(p * width, raw)

    def send_raw(p):
        loads[p][1].wait()
        group = []
        for j in range(1, n_y if p else n_x):
            for which, (buffer, cc) in enumerate(((own, core), (away, 1 - core))):
                if p == 0:
                    t = lax.rem(x + j, n_x)
                    src, dev = buffer.at[:, t, :, raw_span(p)], at(y, t, cc)
                else:
                    t = lax.rem(y + j, n_y)
                    src, dev = buffer.at[t, :, :, raw_span(p)], at(t, x, cc)
                first_dst, other_dst = (r1b, xb) if p else (r1a, xa)
                c = pltpu.make_async_remote_copy(
                    src_ref=src,
                    dst_ref=other_dst.at[j - 1] if which else first_dst.at[0, j - 1, :, :, pl.ds(0, raw)],
                    send_sem=raw_send.at[p, which, j - 1], recv_sem=raw_recv.at[p, which, j - 1],
                    device_id=dev, device_id_type=MESH,
                )
                c.start()
                group.append(c)
        return group

    pair = []
    for p in range(pieces):
        loads[p][0].wait()
        c = pltpu.make_async_remote_copy(
            src_ref=away.at[:, :, :, span(p)], dst_ref=d2d.at[:, :, :, span(p)],
            send_sem=pair_sem.at[0, p], recv_sem=pair_sem.at[1, p],
            device_id=at(y, x, 1 - core), device_id_type=MESH,
        )
        c.start()
        pair.append(c)
        if p == 1:
            raws = [send_raw(0), send_raw(1)]

    ones = []
    for p in range(pieces):
        if p > 1:
            loads[p][1].wait()
        pair[p].wait_recv()
        along_x = p % 2 == 0
        skip = raw if p < 2 else 0
        rest = pl.ds(p * width + skip, width - skip)

        def add_pair(yy, xx, cut):
            total = own[yy, xx, :, cut].astype(jnp.float32) + d2d[yy, xx, :, cut].astype(jnp.float32)
            own[yy, xx, :, cut] = total.astype(jnp.bfloat16)

        def add_all(i, carry, rest=rest):
            add_pair(i // n_x, lax.rem(i, n_x), rest)
            return carry

        lax.fori_loop(0, n_y * n_x, add_all, 0)
        group = []
        for j in range(1, n_x if along_x else n_y):
            landing = pl.ds(skip, width - skip)
            if along_x:
                t = lax.rem(x + j, n_x)
                src, dev = own.at[:, t, :, rest], at(y, t, core)
                dst = r1a.at[p // 2, j - 1, :, :, landing]
            else:
                t = lax.rem(y + j, n_y)
                src, dev = own.at[t, :, :, rest], at(t, x, core)
                dst = r1b.at[p // 2, j - 1, :, :, landing]
            c = pltpu.make_async_remote_copy(
                src_ref=src, dst_ref=dst,
                send_sem=one_send.at[p, j - 1], recv_sem=one_recv.at[p, j - 1],
                device_id=dev, device_id_type=MESH,
            )
            c.start()
            group.append(c)
        ones.append(group)
        if p < 2:
            for i in range(n_y if along_x else n_x):
                add_pair(i if along_x else y, x if along_x else i, raw_span(p))

    twos = []
    for p in range(pieces):
        for c in ones[p]:
            c.wait_recv()
        if p < 2:
            for c in raws[p]:
                c.wait_recv()
            for k in range(n_y - 1 if p else n_x - 1):
                landed, other = (r1b, xb) if p else (r1a, xa)
                total = landed[0, k, :, :, :raw].astype(jnp.float32) + other[k].astype(jnp.float32)
                landed[0, k, :, :, :raw] = total.astype(jnp.bfloat16)
        group = []
        along_x = p % 2 == 0
        for j in range(1, n_y if along_x else n_x):
            if along_x:
                t = lax.rem(y + j, n_y)
                total = own[t, x, :, span(p)].astype(jnp.float32)
                for k in range(n_x - 1):
                    total += r1a[p // 2, k, t].astype(jnp.float32)
                s1a[p // 2, j - 1] = total.astype(jnp.bfloat16)
                src, dst, dev = s1a.at[p // 2, j - 1], r2a.at[p // 2, j - 1], at(t, x, core)
            else:
                t = lax.rem(x + j, n_x)
                total = own[y, t, :, span(p)].astype(jnp.float32)
                for k in range(n_y - 1):
                    total += r1b[p // 2, k, t].astype(jnp.float32)
                s1b[p // 2, j - 1] = total.astype(jnp.bfloat16)
                src, dst, dev = s1b.at[p // 2, j - 1], r2b.at[p // 2, j - 1], at(y, t, core)
            c = pltpu.make_async_remote_copy(
                src_ref=src, dst_ref=dst,
                send_sem=two_send.at[p, j - 1], recv_sem=two_recv.at[p, j - 1],
                device_id=dev, device_id_type=MESH,
            )
            c.start()
            group.append(c)
        twos.append(group)

    def by_block(scalars):
        return jnp.concatenate([jnp.full((block_rows, LANES), s) for s in scalars], axis=0)

    layers = [layer_ref[0, b] for b in range(blocks)]
    lives = [valid_ref[0, b] for b in range(blocks)]
    row_decay = by_block([decay_ref[layer] for layer in layers])
    row_live = by_block([jnp.where(v > 0, 1.0, 0.0).astype(jnp.float32) for v in lives]) > 0.5

    for s in states:
        s.wait()

    zero = jnp.zeros((rows, LANES), jnp.float32)
    sums = (zero, zero)
    for p in range(pieces):
        for c in twos[p]:
            c.wait_recv()
        along_x = p % 2 == 0

        def update_piece(i, sums, p=p, along_x=along_x):
            usum, wsum = sums
            inner = pl.ds(pl.multiple_of(i * LANES, LANES), LANES)
            outer = pl.ds(pl.multiple_of(p * width + i * LANES, LANES), LANES)
            grad = own[y, x, :, outer].astype(jnp.float32)
            if along_x:
                for k in range(n_x - 1):
                    grad += r1a[p // 2, k, y, :, inner].astype(jnp.float32)
                for k in range(n_y - 1):
                    grad += r2a[p // 2, k, :, inner].astype(jnp.float32)
            else:
                for k in range(n_y - 1):
                    grad += r1b[p // 2, k, x, :, inner].astype(jnp.float32)
                for k in range(n_x - 1):
                    grad += r2b[p // 2, k, :, inner].astype(jnp.float32)
            weights = p_v[:, outer].astype(jnp.float32)
            old1, old2 = m1_v[:, outer], m2_v[:, outer]
            first = 0.9 * old1 + 0.1 * grad
            second = 0.99 * old2 + 0.01 * grad * grad
            update = first * (1.0 / bias_first) / (jnp.sqrt(second * (1.0 / bias_second)) + 1e-06) + row_decay * weights
            upd[:, outer] = update
            new1_ref[:, outer] = jnp.where(row_live, first, old1)
            new2_ref[:, outer] = jnp.where(row_live, second, old2)
            return usum + update * update, wsum + weights * weights

        sums = lax.fori_loop(0, width // LANES, update_piece, sums, unroll=2)
        if p < n_sec:
            relay(p + 1)

    for d in range(pieces, n_sec):
        relay(d + 1)

    n_layer = decay_ref.shape[0]
    lane = lax.broadcasted_iota(jnp.int32, (1, LANES), 1)
    line = jnp.zeros((1, LANES), jnp.float32)
    for b in range(blocks):
        chosen = jnp.where(lives[b] > 0, layers[b], -LANES)
        for q, values in enumerate((sums[1], sums[0])):
            part = jnp.sum(values[b * block_rows : (b + 1) * block_rows], axis=0, keepdims=True)
            line += jnp.where(lane == chosen + q * n_layer, jnp.sum(part, axis=1, keepdims=True), 0.0)

    def all_sum(line, slots, send_sem, recv_sem, index, peers):
        slots[index] = line
        copies = []
        for j, peer in enumerate(peers):
            c = pltpu.make_async_remote_copy(
                src_ref=slots.at[index], dst_ref=slots.at[index],
                send_sem=send_sem.at[j], recv_sem=recv_sem.at[j],
                device_id=peer, device_id_type=MESH,
            )
            c.start()
            copies.append(c)
        for c in copies:
            c.wait_recv()
        total = slots[0]
        for j in range(1, len(peers) + 1):
            total += slots[j]
        return total, copies

    shard_peers = [(sec, lax.rem(me + j, n_shard)) for j in range(1, n_shard)]
    sec_peers = [(lax.rem(sec + j, n_sec), me) for j in range(1, n_sec)]
    if ONE_SHOT and n_shard * n_sec <= 32:
        every = [
            (lax.rem(sec + i, n_sec), lax.rem(me + j, n_shard))
            for i in range(n_sec) for j in range(n_shard) if i or j
        ]
        line, sends = all_sum(line, tiles, t_send, t_recv, sec * n_shard + me, every)
    else:
        line, sends = all_sum(line, tiles, t_send, t_recv, me, shard_peers)
        line, zsends = all_sum(line, ztiles, z_send, z_recv, sec, sec_peers)
        sends += zsends
    ratios = jnp.sqrt(line / (pltpu.roll(line, LANES - n_layer, 1) + 1.0))
    ratio_ref[...] = ratios
    step_ref[...] = jnp.concatenate(
        [
            jnp.broadcast_to(
                0.1 * jnp.sum(
                    jnp.where((lane == layers[b]) & (lives[b] > 0), ratios, 0.0), axis=1, keepdims=True
                ),
                (block_rows, LANES),
            )
            for b in range(blocks)
        ],
        axis=0,
    )

    for c in pair + [c for group in raws + ones + twos for c in group] + sends:
        c.wait_send()


def finish(parts, p_v, upd, new1_v, new2_v, step_v, ratio_v, newp_hbm, new1_hbm, new2_hbm, ratio_ref, newp_v, sem):
    cols = p_v.shape[1]
    width = cols // parts
    copies = []
    for k in range(parts):
        span = pl.ds(k * width, width)
        for i, (src, dst) in enumerate(((new1_v, new1_hbm), (new2_v, new2_hbm))):
            c = pltpu.make_async_copy(src.at[:, span], dst.at[:, span], sem.at[i, k])
            c.start()
            copies.append(c)
    ratio_ref[...] = ratio_v[0, : ratio_ref.shape[0]]
    row_step = step_v[...]

    for k in range(parts):
        def step_piece(i, carry, k=k):
            outer = pl.ds(pl.multiple_of(k * width + i * LANES, LANES), LANES)
            stepped = p_v[:, outer].astype(jnp.float32) - row_step * upd[:, outer]
            newp_v[:, outer] = stepped.astype(jnp.bfloat16)
            return carry

        lax.fori_loop(0, width // LANES, step_piece, 0, unroll=4)
        span = pl.ds(k * width, width)
        c = pltpu.make_async_copy(newp_v.at[:, span], newp_hbm.at[:, span], sem.at[2, k])
        c.start()
        copies.append(c)
    for c in copies:
        c.wait()


def shards(grad_parts, params, moment_first, moment_second, block_layer, block_valid, decay):
    n_sec, n_shard = lax.axis_size("section"), lax.axis_size("shard")
    chips = n_shard // 2
    n_y = max(d for d in range(1, math.isqrt(chips) + 1) if chips % d == 0)
    n_x = chips // n_y
    rows, cols = params.shape[1:]
    n_layer = decay.shape[0]
    pieces = PIECES
    half, width = pieces // 2, cols // pieces
    raw = width * 3 // 8 // LANES * LANES
    bf16, f32 = jnp.bfloat16, jnp.float32
    dma = pltpu.SemaphoreType.DMA
    n_lines = n_shard * n_sec if ONE_SHOT and n_shard * n_sec <= 32 else n_shard
    most = max(n_x, n_y) - 1
    grads = grad_parts.reshape(n_y, n_x, 2, rows, cols)
    any_spec = pl.BlockSpec(memory_space=pltpu.HBM)
    smem = pl.BlockSpec(memory_space=pltpu.SMEM)
    vmem = pl.BlockSpec(memory_space=pltpu.VMEM)
    held = pl.pallas_call(
        functools.partial(kernel, n_sec, n_y, n_x, pieces),
        out_shape=(
            pltpu.VMEM((rows, cols), bf16),
            pltpu.VMEM((rows, cols), f32),
            pltpu.VMEM((rows, cols), f32),
            pltpu.VMEM((rows, cols), f32),
            pltpu.VMEM((rows, LANES), f32),
            pltpu.VMEM((1, LANES), f32),
        ),
        in_specs=[any_spec] * 4 + [smem] * 3,
        out_specs=(vmem,) * 6,
        scratch_shapes=[
            pltpu.VMEM((n_y, n_x, rows, cols), bf16),
            pltpu.VMEM((n_y, n_x, rows, cols), bf16),
            pltpu.VMEM((n_y, n_x, rows, cols), bf16),
            pltpu.VMEM((rows, cols), f32),
            pltpu.VMEM((rows, cols), f32),
            pltpu.VMEM((half, n_x - 1, n_y, rows, width), bf16),
            pltpu.VMEM((half, n_y - 1, n_x, rows, width), bf16),
            pltpu.VMEM((half, n_y - 1, rows, width), bf16),
            pltpu.VMEM((half, n_x - 1, rows, width), bf16),
            pltpu.VMEM((half, n_y - 1, rows, width), bf16),
            pltpu.VMEM((half, n_x - 1, rows, width), bf16),
            pltpu.VMEM((n_lines, 1, LANES), f32),
            pltpu.VMEM((n_sec, 1, LANES), f32),
            dma((2, pieces)),
            dma((3,)),
            dma((2, pieces)),
            dma((pieces, most)),
            dma((pieces, most)),
            dma((pieces, most)),
            dma((pieces, most)),
            dma((n_lines - 1,)),
            dma((n_lines - 1,)),
            dma((n_sec - 1,)),
            dma((n_sec - 1,)),
            pltpu.SemaphoreType.REGULAR((2, n_sec - 1)),
            pltpu.VMEM((n_x - 1, n_y, rows, raw), bf16),
            pltpu.VMEM((n_y - 1, n_x, rows, raw), bf16),
            dma((2, 2, most)),
            dma((2, 2, most)),
        ],
        compiler_params=pltpu.CompilerParams(
            collective_id=0, has_side_effects=True, vmem_limit_bytes=56 * 1024 * 1024
        ),
    )(grads, params[0], moment_first[0], moment_second[0], block_layer, block_valid, decay)
    out = pl.pallas_call(
        functools.partial(finish, PARTS),
        out_shape=(
            jax.ShapeDtypeStruct((rows, cols), bf16),
            jax.ShapeDtypeStruct((rows, cols), f32),
            jax.ShapeDtypeStruct((rows, cols), f32),
            jax.ShapeDtypeStruct((n_layer,), f32),
        ),
        in_specs=[vmem] * 6,
        out_specs=(any_spec, any_spec, any_spec, vmem),
        scratch_shapes=[pltpu.VMEM((rows, cols), bf16), dma((3, PARTS))],
        compiler_params=pltpu.CompilerParams(vmem_limit_bytes=8 * 1024 * 1024),
    )(*held)
    return (out[0][None], out[1][None], out[2][None], out[3])


def solution(mesh):
    placed = (
        P("section", "shard", None, None),
        P("section", "shard", None),
        P("section", "shard", None),
        P("section", "shard", None),
        P("section", "shard"),
        P("section", "shard"),
        P(),
    )
    return jax.shard_map(
        shards,
        mesh=mesh,
        in_specs=placed,
        out_specs=(
            P("section", "shard", None),
            P("section", "shard", None),
            P("section", "shard", None),
            P(),
        ),
        check_vma=False,
    )
```

```python
import functools
import math

import jax
import jax.numpy as jnp
from jax import lax
from jax.experimental import pallas as pl
from jax.experimental.pallas import tpu as pltpu
from jax.sharding import PartitionSpec as P

MESH = pl.DeviceIdType.MESH
bias_first = 1.0 - 0.9**10
bias_second = 1.0 - 0.99**10
LANES = 128
PIECES = 8
ONE_SHOT = True
PARTS = 2


def kernel(
    n_sec, n_y, n_x, pieces,
    g_hbm, p_hbm, m1_hbm, m2_hbm, layer_ref, valid_ref, decay_ref,
    p_v, upd, new1_ref, new2_ref, step_ref, ratio_ref,
    own, away, d2d, m1_v, m2_v, r1a, r1b, s1a, s1b, r2a, r2b, tiles, ztiles,
    load_sem, state_sem, pair_sem, one_send, one_recv, two_send, two_recv,
    t_send, t_recv, z_send, z_recv, told, xa, xb, raw_send, raw_recv,
):
    rows, cols = p_v.shape
    width = cols // pieces
    raw = xa.shape[-1]
    n_shard = 2 * n_y * n_x
    sec, me = lax.axis_index("section"), lax.axis_index("shard")
    core = lax.rem(me, 2)
    x = lax.rem(me // 2, n_x)
    y = me // (2 * n_x)
    blocks = layer_ref.shape[1]
    block_rows = rows // blocks

    def at(yy, xx, cc):
        return (sec, (yy * n_x + xx) * 2 + cc)

    def span(p):
        return pl.ds(p * width, width)

    loads = []
    for p in range(pieces):
        a = pltpu.make_async_copy(g_hbm.at[:, :, 1 - core, :, span(p)], away.at[:, :, :, span(p)], load_sem.at[0, p])
        b = pltpu.make_async_copy(g_hbm.at[:, :, core, :, span(p)], own.at[:, :, :, span(p)], load_sem.at[1, p])
        a.start()
        b.start()
        loads.append((a, b))
    states = [
        pltpu.make_async_copy(src, dst, state_sem.at[i])
        for i, (src, dst) in enumerate(((p_hbm, p_v), (m1_hbm, m1_v), (m2_hbm, m2_v)))
    ]
    for s in states:
        s.start()

    barrier = pltpu.get_barrier_semaphore()
    near = [at(y, x, 1 - core)]
    for cc in (core, 1 - core):
        near += [at(y, lax.rem(x + j, n_x), cc) for j in range(1, n_x)]
        near += [at(lax.rem(y + j, n_y), x, cc) for j in range(1, n_y)]
    for peer in near:
        pl.semaphore_signal(barrier, inc=1, device_id=peer, device_id_type=MESH)
    last_sec = n_sec - 1
    up = (jnp.minimum(sec + 1, last_sec), me)
    down = (jnp.maximum(sec - 1, 0), me)

    @pl.when(sec < last_sec)
    def _():
        pl.semaphore_signal(barrier, inc=1, device_id=up, device_id_type=MESH)

    @pl.when(sec > 0)
    def _():
        pl.semaphore_signal(barrier, inc=1, device_id=down, device_id_type=MESH)

    ends = jnp.where(sec < last_sec, 1, 0) + jnp.where(sec > 0, 1, 0)
    pl.semaphore_wait(barrier, len(near) + ends)

    def relay(d):
        if d > 1:

            @pl.when(sec >= d - 1)
            def _():
                pl.semaphore_wait(told.at[0, d - 2], 1)

            @pl.when(sec <= n_sec - d)
            def _():
                pl.semaphore_wait(told.at[1, d - 2], 1)

        if d < n_sec:

            @pl.when((sec >= d - 1) & (sec < last_sec))
            def _():
                pl.semaphore_signal(told.at[0, d - 1], inc=1, device_id=up, device_id_type=MESH)

            @pl.when((sec <= n_sec - d) & (sec > 0))
            def _():
                pl.semaphore_signal(told.at[1, d - 1], inc=1, device_id=down, device_id_type=MESH)

    def raw_span(p):
        return pl.ds(p * width, raw)

    def send_raw(p):
        loads[p][1].wait()
        group = []
        for j in range(1, n_y if p else n_x):
            for which, (buffer, cc) in enumerate(((own, core), (away, 1 - core))):
                if p == 0:
                    t = lax.rem(x + j, n_x)
                    src, dev = buffer.at[:, t, :, raw_span(p)], at(y, t, cc)
                else:
                    t = lax.rem(y + j, n_y)
                    src, dev = buffer.at[t, :, :, raw_span(p)], at(t, x, cc)
                first_dst, other_dst = (r1b, xb) if p else (r1a, xa)
                c = pltpu.make_async_remote_copy(
                    src_ref=src,
                    dst_ref=other_dst.at[j - 1] if which else first_dst.at[0, j - 1, :, :, pl.ds(0, raw)],
                    send_sem=raw_send.at[p, which, j - 1], recv_sem=raw_recv.at[p, which, j - 1],
                    device_id=dev, device_id_type=MESH,
                )
                c.start()
                group.append(c)
        return group

    pair = []
    for p in range(pieces):
        loads[p][0].wait()
        c = pltpu.make_async_remote_copy(
            src_ref=away.at[:, :, :, span(p)], dst_ref=d2d.at[:, :, :, span(p)],
            send_sem=pair_sem.at[0, p], recv_sem=pair_sem.at[1, p],
            device_id=at(y, x, 1 - core), device_id_type=MESH,
        )
        c.start()
        pair.append(c)
        if p == 1:
            raws = [send_raw(0), send_raw(1)]

    ones = []
    for p in range(pieces):
        if p > 1:
            loads[p][1].wait()
        pair[p].wait_recv()
        along_x = p % 2 == 0
        skip = raw if p < 2 else 0
        rest = pl.ds(p * width + skip, width - skip)

        def add_pair(yy, xx, cut):
            total = own[yy, xx, :, cut].astype(jnp.float32) + d2d[yy, xx, :, cut].astype(jnp.float32)
            own[yy, xx, :, cut] = total.astype(jnp.bfloat16)

        def add_all(i, carry, rest=rest):
            add_pair(i // n_x, lax.rem(i, n_x), rest)
            return carry

        lax.fori_loop(0, n_y * n_x, add_all, 0)
        group = []
        for j in range(1, n_x if along_x else n_y):
            landing = pl.ds(skip, width - skip)
            if along_x:
                t = lax.rem(x + j, n_x)
                src, dev = own.at[:, t, :, rest], at(y, t, core)
                dst = r1a.at[p // 2, j - 1, :, :, landing]
            else:
                t = lax.rem(y + j, n_y)
                src, dev = own.at[t, :, :, rest], at(t, x, core)
                dst = r1b.at[p // 2, j - 1, :, :, landing]
            c = pltpu.make_async_remote_copy(
                src_ref=src, dst_ref=dst,
                send_sem=one_send.at[p, j - 1], recv_sem=one_recv.at[p, j - 1],
                device_id=dev, device_id_type=MESH,
            )
            c.start()
            group.append(c)
        ones.append(group)
        if p < 2:
            for i in range(n_y if along_x else n_x):
                add_pair(i if along_x else y, x if along_x else i, raw_span(p))

    twos = []
    for p in range(pieces):
        for c in ones[p]:
            c.wait_recv()
        if p < 2:
            for c in raws[p]:
                c.wait_recv()
            for k in range(n_y - 1 if p else n_x - 1):
                landed, other = (r1b, xb) if p else (r1a, xa)
                total = landed[0, k, :, :, :raw].astype(jnp.float32) + other[k].astype(jnp.float32)
                landed[0, k, :, :, :raw] = total.astype(jnp.bfloat16)
        group = []
        along_x = p % 2 == 0
        for j in range(1, n_y if along_x else n_x):
            if along_x:
                t = lax.rem(y + j, n_y)
                total = own[t, x, :, span(p)].astype(jnp.float32)
                for k in range(n_x - 1):
                    total += r1a[p // 2, k, t].astype(jnp.float32)
                s1a[p // 2, j - 1] = total.astype(jnp.bfloat16)
                src, dst, dev = s1a.at[p // 2, j - 1], r2a.at[p // 2, j - 1], at(t, x, core)
            else:
                t = lax.rem(x + j, n_x)
                total = own[y, t, :, span(p)].astype(jnp.float32)
                for k in range(n_y - 1):
                    total += r1b[p // 2, k, t].astype(jnp.float32)
                s1b[p // 2, j - 1] = total.astype(jnp.bfloat16)
                src, dst, dev = s1b.at[p // 2, j - 1], r2b.at[p // 2, j - 1], at(y, t, core)
            c = pltpu.make_async_remote_copy(
                src_ref=src, dst_ref=dst,
                send_sem=two_send.at[p, j - 1], recv_sem=two_recv.at[p, j - 1],
                device_id=dev, device_id_type=MESH,
            )
            c.start()
            group.append(c)
        twos.append(group)

    def by_block(scalars):
        return jnp.concatenate([jnp.full((block_rows, LANES), s) for s in scalars], axis=0)

    layers = [layer_ref[0, b] for b in range(blocks)]
    lives = [valid_ref[0, b] for b in range(blocks)]
    row_decay = by_block([decay_ref[layer] for layer in layers])
    row_live = by_block([jnp.where(v > 0, 1.0, 0.0).astype(jnp.float32) for v in lives]) > 0.5

    for s in states:
        s.wait()

    zero = jnp.zeros((rows, LANES), jnp.float32)
    sums = (zero, zero)
    for p in range(pieces):
        for c in twos[p]:
            c.wait_recv()
        along_x = p % 2 == 0

        def update_piece(i, sums, p=p, along_x=along_x):
            usum, wsum = sums
            inner = pl.ds(pl.multiple_of(i * LANES, LANES), LANES)
            outer = pl.ds(pl.multiple_of(p * width + i * LANES, LANES), LANES)
            grad = own[y, x, :, outer].astype(jnp.float32)
            if along_x:
                for k in range(n_x - 1):
                    grad += r1a[p // 2, k, y, :, inner].astype(jnp.float32)
                for k in range(n_y - 1):
                    grad += r2a[p // 2, k, :, inner].astype(jnp.float32)
            else:
                for k in range(n_y - 1):
                    grad += r1b[p // 2, k, x, :, inner].astype(jnp.float32)
                for k in range(n_x - 1):
                    grad += r2b[p // 2, k, :, inner].astype(jnp.float32)
            weights = p_v[:, outer].astype(jnp.float32)
            old1, old2 = m1_v[:, outer], m2_v[:, outer]
            first = 0.9 * old1 + 0.1 * grad
            second = 0.99 * old2 + 0.01 * grad * grad
            update = first * (1.0 / bias_first) / (jnp.sqrt(second * (1.0 / bias_second)) + 1e-06) + row_decay * weights
            upd[:, outer] = update
            new1_ref[:, outer] = jnp.where(row_live, first, old1)
            new2_ref[:, outer] = jnp.where(row_live, second, old2)
            return usum + update * update, wsum + weights * weights

        sums = lax.fori_loop(0, width // LANES, update_piece, sums, unroll=2)
        if p < n_sec:
            relay(p + 1)

    for d in range(pieces, n_sec):
        relay(d + 1)

    n_layer = decay_ref.shape[0]
    lane = lax.broadcasted_iota(jnp.int32, (1, LANES), 1)
    lines = []
    for b in range(blocks):
        chosen = jnp.where(lives[b] > 0, layers[b], -LANES)
        for q, values in enumerate((sums[1], sums[0])):
            block = values[b * block_rows : (b + 1) * block_rows]
            lines.append(jnp.where(lane == chosen + q * n_layer, jnp.sum(block, axis=1, keepdims=True), 0.0))
    line = jnp.sum(sum(lines[1:], lines[0]), axis=0, keepdims=True)

    def all_sum(line, slots, send_sem, recv_sem, index, peers):
        slots[index] = line
        copies = []
        for j, peer in enumerate(peers):
            c = pltpu.make_async_remote_copy(
                src_ref=slots.at[index], dst_ref=slots.at[index],
                send_sem=send_sem.at[j], recv_sem=recv_sem.at[j],
                device_id=peer, device_id_type=MESH,
            )
            c.start()
            copies.append(c)
        for c in copies:
            c.wait_recv()
        total = slots[0]
        for j in range(1, len(peers) + 1):
            total += slots[j]
        return total, copies

    shard_peers = [(sec, lax.rem(me + j, n_shard)) for j in range(1, n_shard)]
    sec_peers = [(lax.rem(sec + j, n_sec), me) for j in range(1, n_sec)]
    if ONE_SHOT and n_shard * n_sec <= 32:
        every = [
            (lax.rem(sec + i, n_sec), lax.rem(me + j, n_shard))
            for i in range(n_sec) for j in range(n_shard) if i or j
        ]
        line, sends = all_sum(line, tiles, t_send, t_recv, sec * n_shard + me, every)
    else:
        line, sends = all_sum(line, tiles, t_send, t_recv, me, shard_peers)
        line, zsends = all_sum(line, ztiles, z_send, z_recv, sec, sec_peers)
        sends += zsends
    ratios = jnp.sqrt(line / (pltpu.roll(line, LANES - n_layer, 1) + 1.0))
    ratio_ref[...] = ratios
    step_ref[...] = jnp.concatenate(
        [
            jnp.broadcast_to(
                0.1 * jnp.sum(
                    jnp.where((lane == layers[b]) & (lives[b] > 0), ratios, 0.0), axis=1, keepdims=True
                ),
                (block_rows, LANES),
            )
            for b in range(blocks)
        ],
        axis=0,
    )

    for c in pair + [c for group in raws + ones + twos for c in group] + sends:
        c.wait_send()


def finish(parts, p_v, upd, new1_v, new2_v, step_v, ratio_v, newp_hbm, new1_hbm, new2_hbm, ratio_ref, newp_v, sem):
    cols = p_v.shape[1]
    width = cols // parts
    copies = []
    for k in range(parts):
        span = pl.ds(k * width, width)
        for i, (src, dst) in enumerate(((new1_v, new1_hbm), (new2_v, new2_hbm))):
            c = pltpu.make_async_copy(src.at[:, span], dst.at[:, span], sem.at[i, k])
            c.start()
            copies.append(c)
    ratio_ref[...] = ratio_v[0, : ratio_ref.shape[0]]
    row_step = step_v[...]

    for k in range(parts):
        def step_piece(i, carry, k=k):
            outer = pl.ds(pl.multiple_of(k * width + i * LANES, LANES), LANES)
            stepped = p_v[:, outer].astype(jnp.float32) - row_step * upd[:, outer]
            newp_v[:, outer] = stepped.astype(jnp.bfloat16)
            return carry

        lax.fori_loop(0, width // LANES, step_piece, 0, unroll=4)
        span = pl.ds(k * width, width)
        c = pltpu.make_async_copy(newp_v.at[:, span], newp_hbm.at[:, span], sem.at[2, k])
        c.start()
        copies.append(c)
    for c in copies:
        c.wait()


def shards(grad_parts, params, moment_first, moment_second, block_layer, block_valid, decay):
    n_sec, n_shard = lax.axis_size("section"), lax.axis_size("shard")
    chips = n_shard // 2
    n_y = max(d for d in range(1, math.isqrt(chips) + 1) if chips % d == 0)
    n_x = chips // n_y
    rows, cols = params.shape[1:]
    n_layer = decay.shape[0]
    pieces = PIECES
    half, width = pieces // 2, cols // pieces
    raw = width * 3 // 8 // LANES * LANES
    bf16, f32 = jnp.bfloat16, jnp.float32
    dma = pltpu.SemaphoreType.DMA
    n_lines = n_shard * n_sec if ONE_SHOT and n_shard * n_sec <= 32 else n_shard
    most = max(n_x, n_y) - 1
    grads = grad_parts.reshape(n_y, n_x, 2, rows, cols)
    any_spec = pl.BlockSpec(memory_space=pltpu.HBM)
    smem = pl.BlockSpec(memory_space=pltpu.SMEM)
    vmem = pl.BlockSpec(memory_space=pltpu.VMEM)
    held = pl.pallas_call(
        functools.partial(kernel, n_sec, n_y, n_x, pieces),
        out_shape=(
            pltpu.VMEM((rows, cols), bf16),
            pltpu.VMEM((rows, cols), f32),
            pltpu.VMEM((rows, cols), f32),
            pltpu.VMEM((rows, cols), f32),
            pltpu.VMEM((rows, LANES), f32),
            pltpu.VMEM((1, LANES), f32),
        ),
        in_specs=[any_spec] * 4 + [smem] * 3,
        out_specs=(vmem,) * 6,
        scratch_shapes=[
            pltpu.VMEM((n_y, n_x, rows, cols), bf16),
            pltpu.VMEM((n_y, n_x, rows, cols), bf16),
            pltpu.VMEM((n_y, n_x, rows, cols), bf16),
            pltpu.VMEM((rows, cols), f32),
            pltpu.VMEM((rows, cols), f32),
            pltpu.VMEM((half, n_x - 1, n_y, rows, width), bf16),
            pltpu.VMEM((half, n_y - 1, n_x, rows, width), bf16),
            pltpu.VMEM((half, n_y - 1, rows, width), bf16),
            pltpu.VMEM((half, n_x - 1, rows, width), bf16),
            pltpu.VMEM((half, n_y - 1, rows, width), bf16),
            pltpu.VMEM((half, n_x - 1, rows, width), bf16),
            pltpu.VMEM((n_lines, 1, LANES), f32),
            pltpu.VMEM((n_sec, 1, LANES), f32),
            dma((2, pieces)),
            dma((3,)),
            dma((2, pieces)),
            dma((pieces, most)),
            dma((pieces, most)),
            dma((pieces, most)),
            dma((pieces, most)),
            dma((n_lines - 1,)),
            dma((n_lines - 1,)),
            dma((n_sec - 1,)),
            dma((n_sec - 1,)),
            pltpu.SemaphoreType.REGULAR((2, n_sec - 1)),
            pltpu.VMEM((n_x - 1, n_y, rows, raw), bf16),
            pltpu.VMEM((n_y - 1, n_x, rows, raw), bf16),
            dma((2, 2, most)),
            dma((2, 2, most)),
        ],
        compiler_params=pltpu.CompilerParams(
            collective_id=0, has_side_effects=True, vmem_limit_bytes=56 * 1024 * 1024
        ),
    )(grads, params[0], moment_first[0], moment_second[0], block_layer, block_valid, decay)
    out = pl.pallas_call(
        functools.partial(finish, PARTS),
        out_shape=(
            jax.ShapeDtypeStruct((rows, cols), bf16),
            jax.ShapeDtypeStruct((rows, cols), f32),
            jax.ShapeDtypeStruct((rows, cols), f32),
            jax.ShapeDtypeStruct((n_layer,), f32),
        ),
        in_specs=[vmem] * 6,
        out_specs=(any_spec, any_spec, any_spec, vmem),
        scratch_shapes=[pltpu.VMEM((rows, cols), bf16), dma((3, PARTS))],
        compiler_params=pltpu.CompilerParams(vmem_limit_bytes=8 * 1024 * 1024),
    )(*held)
    return (out[0][None], out[1][None], out[2][None], out[3])


def solution(mesh):
    placed = (
        P("section", "shard", None, None),
        P("section", "shard", None),
        P("section", "shard", None),
        P("section", "shard", None),
        P("section", "shard"),
        P("section", "shard"),
        P(),
    )
    return jax.shard_map(
        shards,
        mesh=mesh,
        in_specs=placed,
        out_specs=(
            P("section", "shard", None),
            P("section", "shard", None),
            P("section", "shard", None),
            P(),
        ),
        check_vma=False,
    )
```
